32 devices in a mesh: dp: 4 (over x, y), tp: 8 (over z, core).
Axes of the slice: x: 2, y: 2, z: 4, core: 2. Of those that a mesh axis runs over, the one named last changes fastest.
Arguments:
- hidden: bfloat16 [4, 512, 4096], P('dp', 'tp'), parts along dimension 0
- vision: bfloat16 [4, 8192, 4096], P('dp', 'tp'), parts along dimension 0
- positions: int32 [4, 512], P('dp', 'tp'), parts along dimension 0
- tile_mask: int32 [4, 512, 4], P('dp', 'tp'), parts along dimension 0
- ln1_a: bfloat16 [4096], replicated
- wq_a: bfloat16 [4096, 4096], P(None, 'tp')
- wk_a: bfloat16 [4096, 1024], P(None, 'tp')
- wv_a: bfloat16 [4096, 1024], P(None, 'tp')
- wo_a: bfloat16 [4096, 4096], P('tp')
- ln2_a: bfloat16 [4096], replicated
- wg_a: bfloat16 [4096, 14336], P(None, 'tp')
- wu_a: bfloat16 [4096, 14336], P(None, 'tp')
- wd_a: bfloat16 [14336, 4096], P('tp')
- ln1_b: bfloat16 [4096], replicated
- wq_b: bfloat16 [4096, 4096], P(None, 'tp')
- q_norm: bfloat16 [128], replicated
- wk_b: bfloat16 [4096, 1024], P(None, 'tp')
- wv_b: bfloat16 [4096, 1024], P(None, 'tp')
- k_norm: bfloat16 [128], replicated
- wo_b: bfloat16 [4096, 4096], P('tp')
- ln2_b: bfloat16 [4096], replicated
- wg_b: bfloat16 [4096, 14336], P(None, 'tp')
- wu_b: bfloat16 [4096, 14336], P(None, 'tp')
- wd_b: bfloat16 [14336, 4096], P('tp')
- xgates: float32 [2], replicated
Outputs:
- output: bfloat16 [4, 512, 4096], P('dp', 'tp'), parts along dimension 0
There are 4 independent parts. The reference program is written for one: setup_inputs(seed, part) draws one part's arguments, and reference() takes and returns one part's arrays. A program takes and returns all parts, laid end to end along the dimension named above; an argument that names none is the same for every part.
All inputs are finite; a program needn't handle non-finite values.
Results may differ from the reference program's by a relative error of at most 0.0167124.
Values are sent between devices in bfloat16 or wider.
A program may use at most 1 GiB of HBM per device.

```python
import math
import jax
import jax.numpy as jnp
from jax import lax

SAMPLES = 1
TOKENS = 512
VISION_TOKENS = 8192
MODEL_DIM = 4096
NUM_HEADS = 32
KV_HEADS = 8
HEAD_DIM = 128
FFN_DIM = 14336
NUM_TILES = 4

ROPE_THETA = 500000.0
ROPE_FACTOR = 8.0
LOW_FACTOR = 1.0
HIGH_FACTOR = 4.0
ORIG_CONTEXT = 8192.0
NORM_EPS = 1e-5
MASK_VALUE = -1e30


def rope_table(head_dim):
    low_wave = ORIG_CONTEXT / LOW_FACTOR
    high_wave = ORIG_CONTEXT / HIGH_FACTOR
    freq_list = []
    for freq_idx in range(head_dim // 2):
        base_freq = 1.0 / (ROPE_THETA ** (2.0 * freq_idx / head_dim))
        wave_len = 2.0 * math.pi / base_freq
        if wave_len > low_wave:
            freq_list.append(base_freq / ROPE_FACTOR)
        elif wave_len < high_wave:
            freq_list.append(base_freq)
        else:
            smooth = (ORIG_CONTEXT / wave_len - LOW_FACTOR) / (HIGH_FACTOR - LOW_FACTOR)
            freq_list.append((1.0 - smooth) * base_freq / ROPE_FACTOR + smooth * base_freq)
    return jnp.array(freq_list, dtype=jnp.float32)


def rms_scale(values, norm_gain):
    values = values.astype(jnp.float32)
    mean_sq = jnp.mean(values * values, axis=-1, keepdims=True)
    return values * lax.rsqrt(mean_sq + NORM_EPS) * norm_gain.astype(jnp.float32)


def rotate(values, cos_tab, sin_tab):
    half_dim = values.shape[-1] // 2
    first_half = values[..., :half_dim]
    second_half = values[..., half_dim:]
    return jnp.concatenate([first_half * cos_tab - second_half * sin_tab, second_half * cos_tab + first_half * sin_tab], axis=-1)


def group_attention(queries, key_vecs, val_vecs, allowed):
    def one_group(operands):
        query_grp, key_grp, val_grp = operands
        scores = jnp.einsum('rqd,kd->rqk', query_grp.astype(jnp.float32), key_grp.astype(jnp.float32)) * (HEAD_DIM ** -0.5)
        weights = jax.nn.softmax(jnp.where(allowed[None], scores, MASK_VALUE), axis=-1).astype(jnp.bfloat16)
        return jnp.einsum('rqk,kd->rqd', weights.astype(jnp.float32), val_grp.astype(jnp.float32)).astype(jnp.bfloat16)
    grouped = lax.map(one_group, (jnp.transpose(queries, (1, 2, 0, 3)), jnp.transpose(key_vecs, (1, 0, 2)), jnp.transpose(val_vecs, (1, 0, 2))))
    return jnp.transpose(grouped, (2, 0, 1, 3)).reshape(queries.shape[0], -1)


def gated_mlp(resid, norm_gain, w_gate, w_up, w_down):
    normed = rms_scale(resid, norm_gain).astype(jnp.bfloat16)
    gate_proj = jnp.dot(normed, w_gate, preferred_element_type=jnp.float32)
    up_proj = jnp.dot(normed, w_up, preferred_element_type=jnp.float32)
    activated = (jax.nn.silu(gate_proj) * up_proj).astype(jnp.bfloat16)
    return jnp.dot(activated, w_down, preferred_element_type=jnp.float32)


def setup_inputs(seed: int = 0, part: int = 0) -> dict:
    data_keys = jax.random.split(jax.random.fold_in(jax.random.key(seed + 1), part), 6)
    weight_keys = jax.random.split(jax.random.key(seed), 22)
    qk_scale = max(math.log(TOKENS / 8.0), 1.0) ** 0.25
    cross_gain = max(math.log(VISION_TOKENS / 16.0), 1.0) ** 0.25
    q_width = NUM_HEADS * HEAD_DIM
    kv_width = KV_HEADS * HEAD_DIM
    dim_scale = MODEL_DIM ** -0.5

    def draw_normal(key_val, arr_shape, spread):
        return (jax.random.normal(key_val, arr_shape, jnp.float32) * spread).astype(jnp.bfloat16)

    def draw_gain(key_val, arr_shape, center):
        return (center * (1.0 + 0.2 * jax.random.normal(key_val, arr_shape, jnp.float32))).astype(jnp.bfloat16)

    hidden = draw_normal(data_keys[0], (SAMPLES, TOKENS, MODEL_DIM), 1.0)
    vision = draw_normal(data_keys[1], (SAMPLES, VISION_TOKENS, MODEL_DIM), 1.0)
    pos_steps = jax.random.randint(data_keys[2], (SAMPLES, TOKENS), 1, 4, dtype=jnp.int32)
    offsets = jax.random.randint(data_keys[3], (SAMPLES, 1), 0, TOKENS, dtype=jnp.int32)
    positions = (offsets + jnp.cumsum(pos_steps, axis=1)).astype(jnp.int32)
    begins = jax.random.randint(data_keys[4], (SAMPLES, 1, 1), 0, TOKENS // 4 + 1, dtype=jnp.int32)
    tile_bits = jax.random.randint(data_keys[5], (SAMPLES, TOKENS, NUM_TILES), 0, 2, dtype=jnp.int32)
    tile_mask = jnp.where(jnp.arange(TOKENS, dtype=jnp.int32)[None, :, None] >= begins, tile_bits, 0).astype(jnp.int32)
    magnitudes = jax.random.uniform(weight_keys[20], (2,), jnp.float32, 0.6, 1.4)
    gate_signs = (2 * jax.random.randint(weight_keys[21], (2,), 0, 2, dtype=jnp.int32) - 1).astype(jnp.float32)
    return {
        'hidden': hidden,
        'vision': vision,
        'positions': positions,
        'tile_mask': tile_mask,
        'ln1_a': draw_gain(weight_keys[0], (MODEL_DIM,), 1.0),
        'wq_a': draw_normal(weight_keys[1], (MODEL_DIM, q_width), qk_scale * dim_scale),
        'wk_a': draw_normal(weight_keys[2], (MODEL_DIM, kv_width), qk_scale * dim_scale),
        'wv_a': draw_normal(weight_keys[3], (MODEL_DIM, kv_width), dim_scale),
        'wo_a': draw_normal(weight_keys[4], (q_width, MODEL_DIM), q_width ** -0.5),
        'ln2_a': draw_gain(weight_keys[5], (MODEL_DIM,), 1.0),
        'wg_a': draw_normal(weight_keys[6], (MODEL_DIM, FFN_DIM), dim_scale),
        'wu_a': draw_normal(weight_keys[7], (MODEL_DIM, FFN_DIM), dim_scale),
        'wd_a': draw_normal(weight_keys[8], (FFN_DIM, MODEL_DIM), FFN_DIM ** -0.5),
        'ln1_b': draw_gain(weight_keys[9], (MODEL_DIM,), 1.0),
        'wq_b': draw_normal(weight_keys[10], (MODEL_DIM, q_width), dim_scale),
        'q_norm': draw_gain(weight_keys[11], (HEAD_DIM,), cross_gain),
        'wk_b': draw_normal(weight_keys[12], (MODEL_DIM, kv_width), dim_scale),
        'wv_b': draw_normal(weight_keys[13], (MODEL_DIM, kv_width), dim_scale),
        'k_norm': draw_gain(weight_keys[14], (HEAD_DIM,), cross_gain),
        'wo_b': draw_normal(weight_keys[15], (q_width, MODEL_DIM), q_width ** -0.5),
        'ln2_b': draw_gain(weight_keys[16], (MODEL_DIM,), 1.0),
        'wg_b': draw_normal(weight_keys[17], (MODEL_DIM, FFN_DIM), dim_scale),
        'wu_b': draw_normal(weight_keys[18], (MODEL_DIM, FFN_DIM), dim_scale),
        'wd_b': draw_normal(weight_keys[19], (FFN_DIM, MODEL_DIM), FFN_DIM ** -0.5),
        'xgates': magnitudes * gate_signs,
    }


def reference(hidden, vision, positions, tile_mask, ln1_a, wq_a, wk_a, wv_a, wo_a, ln2_a, wg_a, wu_a, wd_a, ln1_b, wq_b, q_norm, wk_b, wv_b, k_norm, wo_b, ln2_b, wg_b, wu_b, wd_b, xgates):
    rep_heads = NUM_HEADS // KV_HEADS
    tile_len = VISION_TOKENS // NUM_TILES
    inv_freq = rope_table(HEAD_DIM)
    gate_vals = jnp.tanh(xgates.astype(jnp.float32))
    causal = lax.broadcasted_iota(jnp.int32, (TOKENS, TOKENS), 0) >= lax.broadcasted_iota(jnp.int32, (TOKENS, TOKENS), 1)

    def one_sample(operands):
        hid_rows, vis_rows, pos_row, mask_row = operands
        angles = pos_row.astype(jnp.float32)[:, None] * inv_freq[None, :]
        cos_tab = jnp.cos(angles)[:, None, :]
        sin_tab = jnp.sin(angles)[:, None, :]
        normed = rms_scale(hid_rows, ln1_a).astype(jnp.bfloat16)
        queries = jnp.dot(normed, wq_a, preferred_element_type=jnp.float32).reshape(TOKENS, NUM_HEADS, HEAD_DIM)
        queries = rotate(queries, cos_tab, sin_tab).astype(jnp.bfloat16).reshape(TOKENS, KV_HEADS, rep_heads, HEAD_DIM)
        key_vecs = jnp.dot(normed, wk_a, preferred_element_type=jnp.float32).reshape(TOKENS, KV_HEADS, HEAD_DIM)
        key_vecs = rotate(key_vecs, cos_tab, sin_tab).astype(jnp.bfloat16)
        val_vecs = jnp.dot(normed, wv_a, preferred_element_type=jnp.float32).astype(jnp.bfloat16).reshape(TOKENS, KV_HEADS, HEAD_DIM)
        context = group_attention(queries, key_vecs, val_vecs, causal)
        h_one = (hid_rows.astype(jnp.float32) + jnp.dot(context, wo_a, preferred_element_type=jnp.float32)).astype(jnp.bfloat16)
        h_two = (h_one.astype(jnp.float32) + gated_mlp(h_one, ln2_a, wg_a, wu_a, wd_a)).astype(jnp.bfloat16)
        normed = rms_scale(h_two, ln1_b).astype(jnp.bfloat16)
        queries = jnp.dot(normed, wq_b, preferred_element_type=jnp.float32).reshape(TOKENS, NUM_HEADS, HEAD_DIM)
        queries = rms_scale(queries, q_norm).astype(jnp.bfloat16).reshape(TOKENS, KV_HEADS, rep_heads, HEAD_DIM)
        key_vecs = jnp.dot(vis_rows, wk_b, preferred_element_type=jnp.float32).reshape(VISION_TOKENS, KV_HEADS, HEAD_DIM)
        key_vecs = rms_scale(key_vecs, k_norm).astype(jnp.bfloat16)
        val_vecs = jnp.dot(vis_rows, wv_b, preferred_element_type=jnp.float32).astype(jnp.bfloat16).reshape(VISION_TOKENS, KV_HEADS, HEAD_DIM)
        visible = mask_row > 0
        allowed = jnp.repeat(visible, tile_len, axis=1)
        context = group_attention(queries, key_vecs, val_vecs, allowed)
        row_keep = jnp.any(visible, axis=-1, keepdims=True).astype(jnp.float32)
        attn_out = jnp.dot(context, wo_b, preferred_element_type=jnp.float32)
        h_three = (h_two.astype(jnp.float32) + gate_vals[0] * row_keep * attn_out).astype(jnp.bfloat16)
        mlp_out = gated_mlp(h_three, ln2_b, wg_b, wu_b, wd_b)
        return (h_three.astype(jnp.float32) + gate_vals[1] * row_keep * mlp_out).astype(jnp.bfloat16)

    return lax.map(one_sample, (hidden, vision, positions, tile_mask))
```

```python
import functools
import math
import jax
import jax.numpy as jnp
from jax import lax
from jax.experimental import pallas as pl
from jax.experimental.pallas import tpu as pltpu
from jax.sharding import PartitionSpec as P

ROPE_THETA = 500000.0
ROPE_FACTOR = 8.0
LOW_FACTOR = 1.0
HIGH_FACTOR = 4.0
ORIG_CONTEXT = 8192.0
NORM_EPS = 1e-5
MASK_VALUE = -1e30
BF16 = jnp.bfloat16
F32 = jnp.float32


def rope_table(head_dim):
    low_wave = ORIG_CONTEXT / LOW_FACTOR
    high_wave = ORIG_CONTEXT / HIGH_FACTOR
    freq_list = []
    for freq_idx in range(head_dim // 2):
        base_freq = 1.0 / (ROPE_THETA ** (2.0 * freq_idx / head_dim))
        wave_len = 2.0 * math.pi / base_freq
        if wave_len > low_wave:
            freq_list.append(base_freq / ROPE_FACTOR)
        elif wave_len < high_wave:
            freq_list.append(base_freq)
        else:
            smooth = (ORIG_CONTEXT / wave_len - LOW_FACTOR) / (HIGH_FACTOR - LOW_FACTOR)
            freq_list.append((1.0 - smooth) * base_freq / ROPE_FACTOR + smooth * base_freq)
    return jnp.array(freq_list, dtype=jnp.float32)


def rms_scale(values, norm_gain):
    values = values.astype(jnp.float32)
    mean_sq = jnp.mean(values * values, axis=-1, keepdims=True)
    return values * lax.rsqrt(mean_sq + NORM_EPS) * norm_gain.astype(jnp.float32)


def rotate(values, cos_tab, sin_tab):
    half_dim = values.shape[-1] // 2
    first_half = values[..., :half_dim]
    second_half = values[..., half_dim:]
    return jnp.concatenate([first_half * cos_tab - second_half * sin_tab, second_half * cos_tab + first_half * sin_tab], axis=-1)


def self_attend(queries, key_vecs, val_vecs):
    seq_len = queries.shape[3]
    head_dim = queries.shape[4]
    scores = jnp.einsum('bgrtd,bsgd->bgrts', queries, key_vecs, preferred_element_type=jnp.float32) * (head_dim ** -0.5)
    causal = lax.broadcasted_iota(jnp.int32, (seq_len, seq_len), 0) >= lax.broadcasted_iota(jnp.int32, (seq_len, seq_len), 1)
    weights = jax.nn.softmax(jnp.where(causal, scores, MASK_VALUE), axis=-1).astype(jnp.bfloat16)
    return jnp.einsum('bgrts,bsgd->bgrtd', weights, val_vecs, preferred_element_type=jnp.float32).astype(jnp.bfloat16)


def gather_rows(values):
    return lax.all_gather(values, 'tp', axis=1, tiled=True)


def scatter_sum(partial):
    return lax.psum_scatter(partial, 'tp', scatter_dimension=1, tiled=True).astype(jnp.float32)


def gated_mlp(resid, norm_gain, w_gate, w_up, w_down):
    gathered = gather_rows(rms_scale(resid, norm_gain).astype(jnp.bfloat16))
    gate_proj = jnp.einsum('btd,df->btf', gathered, w_gate, preferred_element_type=jnp.float32)
    up_proj = jnp.einsum('btd,df->btf', gathered, w_up, preferred_element_type=jnp.float32)
    activated = (jax.nn.silu(gate_proj) * up_proj).astype(jnp.bfloat16)
    partial = jnp.einsum('btf,fd->btd', activated, w_down, preferred_element_type=jnp.float32).astype(jnp.bfloat16)
    return scatter_sum(partial)


def kv_kernel(tab, vis, own, b1, b1s, b2, b2s, d0, d1, d0s, d1s, gain, out, acc):
    rel = pl.program_id(0)
    quarter = own.shape[1]
    dp = tab[0]

    def cols(q):
        return vis[:, pl.ds(pl.multiple_of(q * quarter, quarter), quarter)]

    acc[...] = jnp.dot(cols(dp), own[0], preferred_element_type=F32)

    def add(cond, q, ref):
        @pl.when(cond)
        def _():
            acc[...] += jnp.dot(cols(q), ref[0], preferred_element_type=F32)

    q1, q2, q3 = tab[1], tab[2], tab[3]
    add(rel < 4, q1, b1)
    add(rel >= 4, q1, b1s)
    add(rel < 4, q2, b2)
    add(rel >= 4, q2, b2s)
    add(rel < 2, q3, d0)
    add((rel >= 2) & (rel < 4), q3, d1)
    add((rel >= 4) & (rel < 6), q3, d0s)
    add(rel >= 6, q3, d1s)
    hd = out.shape[2] // 2
    keys = acc[:, :hd]
    mean_sq = jnp.mean(keys * keys, axis=-1, keepdims=True)
    out[0, :, :hd] = (keys * lax.rsqrt(mean_sq + NORM_EPS) * gain[...].astype(F32)).astype(BF16)
    out[0, :, hd:] = acc[:, hd:].astype(BF16)


def kv_call(tab, vision, own, b1, b1s, b2, b2s, d0, d1, d0s, d1s, gain):
    toks, dim = vision.shape
    heads, quarter, width = own.shape

    def clip(lo, n):
        return lambda r, tab: (jnp.clip(r - lo, 0, n - 1), 0, 0)

    wblk = (1, quarter, width)
    grid_spec = pltpu.PrefetchScalarGridSpec(
        num_scalar_prefetch=1,
        grid=(heads,),
        in_specs=[
            pl.BlockSpec((toks, dim), lambda r, tab: (0, 0)),
            pl.BlockSpec(wblk, lambda r, tab: (lax.rem(tab[4] + r, heads), 0, 0)),
            pl.BlockSpec(wblk, clip(0, 4)),
            pl.BlockSpec(wblk, clip(4, 4)),
            pl.BlockSpec(wblk, clip(0, 4)),
            pl.BlockSpec(wblk, clip(4, 4)),
            pl.BlockSpec(wblk, clip(0, 2)),
            pl.BlockSpec(wblk, clip(2, 2)),
            pl.BlockSpec(wblk, clip(4, 2)),
            pl.BlockSpec(wblk, clip(6, 2)),
            pl.BlockSpec((1, width // 2), lambda r, tab: (0, 0)),
        ],
        out_specs=pl.BlockSpec((1, toks, width), lambda r, tab: (lax.rem(tab[5] + r, heads), 0, 0)),
        scratch_shapes=[pltpu.VMEM((toks, width), F32)],
    )
    return pl.pallas_call(
        kv_kernel,
        grid_spec=grid_spec,
        out_shape=jax.ShapeDtypeStruct((heads, toks, width), BF16),
        compiler_params=pltpu.CompilerParams(vmem_limit_bytes=56 * 2**20),
        cost_estimate=pl.CostEstimate(flops=2 * toks * dim * heads * width, bytes_accessed=30 * 2**20, transcendentals=0),
        name="vision_kv",
    )(tab, vision, own, b1, b1s, b2, b2s, d0, d1, d0s, d1s, gain)


def flash_kernel(scale, q_ref, vis_ref, *refs):
    kvs, out = refs[:-1], refs[-1]
    hd = q_ref.shape[1]
    rows = q_ref.shape[0]
    q = q_ref[...]
    m = jnp.full((rows, 1), -jnp.inf, F32)
    l = jnp.zeros((rows, 1), F32)
    acc = jnp.zeros((rows, hd), F32)
    for j, kv in enumerate(kvs):
        s = lax.dot_general(q, kv[:, :hd], (((1,), (1,)), ((), ())), preferred_element_type=F32)
        seen = vis_ref[:, j:j + 1] > 0
        m_new = jnp.where(seen, jnp.maximum(m, jnp.max(s, axis=-1, keepdims=True)), m)
        shift = jnp.where(seen, m_new, 1e30)
        p = jnp.exp2((s - shift) * scale)
        m_fin = jnp.where(m_new == -jnp.inf, 0.0, m_new)
        alpha = jnp.exp2((m - m_fin) * scale)
        l = alpha * l + jnp.sum(p, axis=-1, keepdims=True)
        acc = alpha * acc + jnp.dot(p.astype(BF16), kv[:, hd:], preferred_element_type=F32)
        m = m_new
    out[...] = (acc / jnp.where(l == 0, 1.0, l)).astype(BF16)


def flash_call(queries, seen, kvs):
    toks, width = queries.shape
    n, kw = kvs[0].shape
    hd = kw // 2
    heads = width // hd
    rows = 256
    scale = hd ** -0.5 * math.log2(math.e)
    return pl.pallas_call(
        functools.partial(flash_kernel, scale),
        grid=(toks // rows, heads),
        in_specs=[pl.BlockSpec((rows, hd), lambda i, h: (i, h)), pl.BlockSpec((rows, len(kvs)), lambda i, h: (i, 0))]
        + [pl.BlockSpec((n, kw), lambda i, h: (0, 0))] * len(kvs),
        out_specs=pl.BlockSpec((rows, hd), lambda i, h: (i, h)),
        out_shape=jax.ShapeDtypeStruct((toks, width), BF16),
        compiler_params=pltpu.CompilerParams(vmem_limit_bytes=48 * 2**20),
        cost_estimate=pl.CostEstimate(flops=4 * toks * width * n * len(kvs), bytes_accessed=8 * 2**20, transcendentals=toks * heads * n * len(kvs)),
        name="cross_flash",
    )(queries, seen, *kvs)


def solution(mesh):
    act_spec = P('dp', 'tp', None)
    col_spec = P(None, 'tp')
    row_spec = P('tp', None)
    layer_a = (P(), col_spec, col_spec, col_spec, row_spec, P(), col_spec, col_spec, row_spec)
    layer_b = (P(), col_spec, P(), col_spec, col_spec, P(), row_spec, P(), col_spec, col_spec, row_spec, P())
    in_specs = (act_spec, act_spec, P('dp', 'tp'), act_spec) + layer_a + layer_b
    ndp, ntp = mesh.shape['dp'], mesh.shape['tp']

    def perm(fn):
        pairs = []
        for d in range(ndp):
            for t in range(ntp):
                d2, t2 = fn(d, t)
                pairs.append((d * ntp + t, d2 * ntp + t2))
        return pairs

    def permute(x, fn):
        return lax.ppermute(x, ('dp', 'tp'), perm(fn))

    def body(hidden, vision, positions, tile_mask, ln1_a, wq_a, wk_a, wv_a, wo_a, ln2_a, wg_a, wu_a, wd_a, ln1_b, wq_b, q_norm, wk_b, wv_b, k_norm, wo_b, ln2_b, wg_b, wu_b, wd_b, xgates):
        dp = lax.axis_index('dp')
        tp = lax.axis_index('tp')
        core = tp % 2
        head_dim = q_norm.shape[0]
        model_dim = hidden.shape[2]
        toks_local = hidden.shape[1]
        kv_local = wk_a.shape[1] // head_dim
        rep_heads = wq_a.shape[1] // head_dim // kv_local
        query_shape = (model_dim, kv_local, rep_heads, head_dim)
        head_shape = (model_dim, kv_local, head_dim)
        out_shape = (kv_local, rep_heads, head_dim, model_dim)

        small = jnp.concatenate([positions[0][None], tile_mask[0].T, jnp.zeros((3, toks_local), jnp.int32)], axis=0)
        small = lax.all_gather(small, 'tp', axis=0)
        small = jnp.transpose(small, (1, 0, 2)).reshape(8, ntp * toks_local)
        pos_all = small[0]
        mask_all = small[1:5]

        gathered = gather_rows(rms_scale(hidden, ln1_a).astype(jnp.bfloat16))

        quarter = model_dim // ndp
        w_loc = jnp.concatenate([lax.dynamic_slice_in_dim(wk_b, dp * quarter, quarter, 0), lax.dynamic_slice_in_dim(wv_b, dp * quarter, quarter, 0)], axis=1)
        w_loc, gathered = lax.optimization_barrier((w_loc, gathered))
        w_own = lax.all_gather(w_loc, 'tp', axis=0)
        half = ntp // 2
        w_half = lax.dynamic_slice_in_dim(w_own, core * half, half, 0)
        b1 = permute(w_half, lambda d, t: (d ^ 1, t))
        b2 = permute(w_half, lambda d, t: (d ^ 2, t))
        d0 = permute(b1[:2], lambda d, t: (d ^ 2, t))
        d1 = permute(b2[2:], lambda d, t: (d ^ 1, t))
        sib = lambda d, t: (d, t ^ 1)
        b1s, b2s, d0s, d1s = permute(b1, sib), permute(b2, sib), permute(d0, sib), permute(d1, sib)
        tab = jnp.stack([dp, dp ^ 1, dp ^ 2, dp ^ 3, core * half, (core * half - tp + ntp) % ntp]).astype(jnp.int32)
        kv_all = kv_call(tab, vision[0], w_own, b1, b1s, b2, b2s, d0, d1, d0s, d1s, k_norm[None])
        kvs = [kv_all[0]]
        for j in range(1, ntp):
            kvs.append(permute(kv_all[j], lambda d, t, j=j: (d, (t + j) % ntp)))

        angles = pos_all.astype(jnp.float32)[None, :, None] * rope_table(head_dim)
        cos_tab = jnp.cos(angles)
        sin_tab = jnp.sin(angles)
        queries = jnp.einsum('btd,dgre->bgrte', gathered, wq_a.reshape(query_shape), preferred_element_type=jnp.float32)
        queries = rotate(queries, cos_tab[:, None, None], sin_tab[:, None, None]).astype(jnp.bfloat16)
        key_vecs = jnp.einsum('btd,dge->btge', gathered, wk_a.reshape(head_shape), preferred_element_type=jnp.float32)
        key_vecs = rotate(key_vecs, cos_tab[:, :, None], sin_tab[:, :, None]).astype(jnp.bfloat16)
        val_vecs = jnp.einsum('btd,dge->btge', gathered, wv_a.reshape(head_shape), preferred_element_type=jnp.float32).astype(jnp.bfloat16)
        context = self_attend(queries, key_vecs, val_vecs)
        partial = jnp.einsum('bgrtd,grde->bte', context, wo_a.reshape(out_shape), preferred_element_type=jnp.float32).astype(jnp.bfloat16)
        h_one = (hidden.astype(jnp.float32) + scatter_sum(partial)).astype(jnp.bfloat16)
        h_two = (h_one.astype(jnp.float32) + gated_mlp(h_one, ln2_a, wg_a, wu_a, wd_a)).astype(jnp.bfloat16)

        gathered = gather_rows(rms_scale(h_two, ln1_b).astype(jnp.bfloat16))[0]
        queries = jnp.dot(gathered, wq_b, preferred_element_type=jnp.float32).reshape(-1, rep_heads * kv_local, head_dim)
        queries = rms_scale(queries, q_norm).astype(jnp.bfloat16).reshape(-1, rep_heads * kv_local * head_dim)
        tiles = jnp.stack([((tp - j + ntp) % ntp) // (ntp // 4) for j in range(ntp)])
        seen = (jnp.take(mask_all, tiles, axis=0) > 0).astype(F32).T
        context = flash_call(queries, seen, kvs)
        partial = jnp.dot(context, wo_b, preferred_element_type=jnp.float32).astype(jnp.bfloat16)[None]
        row_keep = jnp.any(tile_mask > 0, axis=-1, keepdims=True).astype(jnp.float32)
        gate_vals = jnp.tanh(xgates.astype(jnp.float32))
        h_three = (h_two.astype(jnp.float32) + gate_vals[0] * row_keep * scatter_sum(partial)).astype(jnp.bfloat16)
        mlp_out = gated_mlp(h_three, ln2_b, wg_b, wu_b, wd_b)
        return (h_three.astype(jnp.float32) + gate_vals[1] * row_keep * mlp_out).astype(jnp.bfloat16)

    return jax.shard_map(body, mesh=mesh, in_specs=in_specs, out_specs=act_spec, check_vma=False)
```

```python
import functools
import math
import jax
import jax.numpy as jnp
from jax import lax
from jax.experimental import pallas as pl
from jax.experimental.pallas import tpu as pltpu
from jax.sharding import PartitionSpec as P

ROPE_THETA = 500000.0
ROPE_FACTOR = 8.0
LOW_FACTOR = 1.0
HIGH_FACTOR = 4.0
ORIG_CONTEXT = 8192.0
NORM_EPS = 1e-5
MASK_VALUE = -1e30
BF16 = jnp.bfloat16
F32 = jnp.float32


def rope_table(head_dim):
    low_wave = ORIG_CONTEXT / LOW_FACTOR
    high_wave = ORIG_CONTEXT / HIGH_FACTOR
    freq_list = []
    for freq_idx in range(head_dim // 2):
        base_freq = 1.0 / (ROPE_THETA ** (2.0 * freq_idx / head_dim))
        wave_len = 2.0 * math.pi / base_freq
        if wave_len > low_wave:
            freq_list.append(base_freq / ROPE_FACTOR)
        elif wave_len < high_wave:
            freq_list.append(base_freq)
        else:
            smooth = (ORIG_CONTEXT / wave_len - LOW_FACTOR) / (HIGH_FACTOR - LOW_FACTOR)
            freq_list.append((1.0 - smooth) * base_freq / ROPE_FACTOR + smooth * base_freq)
    return jnp.array(freq_list, dtype=jnp.float32)


def rms_scale(values, norm_gain):
    values = values.astype(jnp.float32)
    mean_sq = jnp.mean(values * values, axis=-1, keepdims=True)
    return values * lax.rsqrt(mean_sq + NORM_EPS) * norm_gain.astype(jnp.float32)


def rotate(values, cos_tab, sin_tab):
    half_dim = values.shape[-1] // 2
    first_half = values[..., :half_dim]
    second_half = values[..., half_dim:]
    return jnp.concatenate([first_half * cos_tab - second_half * sin_tab, second_half * cos_tab + first_half * sin_tab], axis=-1)


def self_attend(queries, key_vecs, val_vecs):
    seq_len = queries.shape[3]
    head_dim = queries.shape[4]
    scores = jnp.einsum('bgrtd,bsgd->bgrts', queries, key_vecs, preferred_element_type=jnp.float32) * (head_dim ** -0.5)
    causal = lax.broadcasted_iota(jnp.int32, (seq_len, seq_len), 0) >= lax.broadcasted_iota(jnp.int32, (seq_len, seq_len), 1)
    weights = jax.nn.softmax(jnp.where(causal, scores, MASK_VALUE), axis=-1).astype(jnp.bfloat16)
    return jnp.einsum('bgrts,bsgd->bgrtd', weights, val_vecs, preferred_element_type=jnp.float32).astype(jnp.bfloat16)


def gather_rows(values):
    return lax.all_gather(values, 'tp', axis=1, tiled=True)


def scatter_sum(partial):
    return lax.psum_scatter(partial, 'tp', scatter_dimension=1, tiled=True).astype(jnp.float32)


def kv_kernel(tab, vis, own, b1, b1s, b2, b2s, d0, d1, d0s, d1s, gain, out, acc):
    rel = pl.program_id(0)
    quarter = own.shape[1]
    dp = tab[0]

    def cols(q):
        return vis[:, pl.ds(pl.multiple_of(q * quarter, quarter), quarter)]

    acc[...] = jnp.dot(cols(dp), own[0], preferred_element_type=F32)

    def add(cond, q, ref):
        @pl.when(cond)
        def _():
            acc[...] += jnp.dot(cols(q), ref[0], preferred_element_type=F32)

    q1, q2, q3 = tab[1], tab[2], tab[3]
    add(rel < 4, q1, b1)
    add(rel >= 4, q1, b1s)
    add(rel < 4, q2, b2)
    add(rel >= 4, q2, b2s)
    add(rel < 2, q3, d0)
    add((rel >= 2) & (rel < 4), q3, d1)
    add((rel >= 4) & (rel < 6), q3, d0s)
    add(rel >= 6, q3, d1s)
    hd = out.shape[2] // 2
    keys = acc[:, :hd]
    mean_sq = jnp.mean(keys * keys, axis=-1, keepdims=True)
    out[0, :, :hd] = (keys * lax.rsqrt(mean_sq + NORM_EPS) * gain[...].astype(F32)).astype(BF16)
    out[0, :, hd:] = acc[:, hd:].astype(BF16)


def kv_call(tab, vision, own, b1, b1s, b2, b2s, d0, d1, d0s, d1s, gain):
    toks, dim = vision.shape
    heads, quarter, width = own.shape

    def clip(lo, n):
        return lambda r, tab: (jnp.clip(r - lo, 0, n - 1), 0, 0)

    wblk = (1, quarter, width)
    grid_spec = pltpu.PrefetchScalarGridSpec(
        num_scalar_prefetch=1,
        grid=(heads,),
        in_specs=[
            pl.BlockSpec((toks, dim), lambda r, tab: (0, 0)),
            pl.BlockSpec(wblk, lambda r, tab: (lax.rem(tab[4] + r, heads), 0, 0)),
            pl.BlockSpec(wblk, clip(0, 4)),
            pl.BlockSpec(wblk, clip(4, 4)),
            pl.BlockSpec(wblk, clip(0, 4)),
            pl.BlockSpec(wblk, clip(4, 4)),
            pl.BlockSpec(wblk, clip(0, 2)),
            pl.BlockSpec(wblk, clip(2, 2)),
            pl.BlockSpec(wblk, clip(4, 2)),
            pl.BlockSpec(wblk, clip(6, 2)),
            pl.BlockSpec((1, width // 2), lambda r, tab: (0, 0)),
        ],
        out_specs=pl.BlockSpec((1, toks, width), lambda r, tab: (lax.rem(tab[5] + r, heads), 0, 0)),
        scratch_shapes=[pltpu.VMEM((toks, width), F32)],
    )
    return pl.pallas_call(
        kv_kernel,
        grid_spec=grid_spec,
        out_shape=jax.ShapeDtypeStruct((heads, toks, width), BF16),
        compiler_params=pltpu.CompilerParams(vmem_limit_bytes=56 * 2**20),
        cost_estimate=pl.CostEstimate(flops=2 * toks * dim * heads * width, bytes_accessed=30 * 2**20, transcendentals=0),
        name="vision_kv",
    )(tab, vision, own, b1, b1s, b2, b2s, d0, d1, d0s, d1s, gain)


def flash_kernel(scale, q_ref, vis_ref, *refs):
    kvs, out = refs[:-1], refs[-1]
    hd = q_ref.shape[1]
    rows = q_ref.shape[0]
    q = q_ref[...]
    m = jnp.full((rows, 1), -jnp.inf, F32)
    l = jnp.zeros((rows, 1), F32)
    acc = jnp.zeros((rows, hd), F32)
    for j, kv in enumerate(kvs):
        s = lax.dot_general(q, kv[:, :hd], (((1,), (1,)), ((), ())), preferred_element_type=F32)
        seen = vis_ref[:, j:j + 1] > 0
        m_new = jnp.where(seen, jnp.maximum(m, jnp.max(s, axis=-1, keepdims=True)), m)
        shift = jnp.where(seen, m_new, 1e30)
        p = jnp.exp2((s - shift) * scale)
        m_fin = jnp.where(m_new == -jnp.inf, 0.0, m_new)
        alpha = jnp.exp2((m - m_fin) * scale)
        l = alpha * l + jnp.sum(p, axis=-1, keepdims=True)
        acc = alpha * acc + jnp.dot(p.astype(BF16), kv[:, hd:], preferred_element_type=F32)
        m = m_new
    out[...] = (acc / jnp.where(l == 0, 1.0, l)).astype(BF16)


def flash_call(queries, seen, kvs):
    toks, width = queries.shape
    n, kw = kvs[0].shape
    hd = kw // 2
    heads = width // hd
    rows = 256
    scale = hd ** -0.5 * math.log2(math.e)
    return pl.pallas_call(
        functools.partial(flash_kernel, scale),
        grid=(toks // rows, heads),
        in_specs=[pl.BlockSpec((rows, hd), lambda i, h: (i, h)), pl.BlockSpec((rows, len(kvs)), lambda i, h: (i, 0))]
        + [pl.BlockSpec((n, kw), lambda i, h: (0, 0))] * len(kvs),
        out_specs=pl.BlockSpec((rows, hd), lambda i, h: (i, h)),
        out_shape=jax.ShapeDtypeStruct((toks, width), BF16),
        compiler_params=pltpu.CompilerParams(vmem_limit_bytes=48 * 2**20),
        cost_estimate=pl.CostEstimate(flops=4 * toks * width * n * len(kvs), bytes_accessed=8 * 2**20, transcendentals=toks * heads * n * len(kvs)),
        name="cross_flash",
    )(queries, seen, *kvs)


LINE = 4
PIECES = 4


def silu(x):
    return x / (1.0 + jnp.exp(-x))


def mlp_kernel(h_ref, gain_ref, scale_ref, wg_hbm, wu_hbm, wd_hbm, out_ref,
               xbuf, wg, wu, wd, act, pbuf, sibr, rbuf,
               wsem, asend, arecv, psend, precv, csend, crecv):
    t = lax.axis_index("tp")
    c = lax.rem(t, 2)
    z = lax.div(t, 2)
    up_side = z < LINE // 2
    s = jnp.where(up_side, 1, -1)
    is_end = (z == 0) | (z == LINE - 1)
    is_mid = jnp.logical_not(is_end)
    sib = t + 1 - 2 * c
    ahead = t + 2 * s
    behind = t - 2 * s
    dir_a = jnp.where(up_side, 0, 1)
    dir_b = 1 - dir_a

    parts = 4
    def w_copies(src, dst, k):
        n = src.shape[0] // parts
        return [pltpu.make_async_copy(src.at[pl.ds(i * n, n)], dst.at[pl.ds(i * n, n)], wsem.at[k]) for i in range(parts)]
    for k, (src, dst) in enumerate(((wg_hbm, wg), (wu_hbm, wu), (wd_hbm, wd))):
        for cp in w_copies(src, dst, k):
            cp.start()

    def w_wait(src, dst, k):
        pltpu.make_async_copy(src, dst, wsem.at[k]).wait()

    h = h_ref[...].astype(F32)
    mean_sq = jnp.mean(h * h, axis=-1, keepdims=True)
    xbuf[z, c] = (h * lax.rsqrt(mean_sq + NORM_EPS) * gain_ref[...].astype(F32)).astype(BF16)

    barrier = pltpu.get_barrier_semaphore()
    for peer in (sib, ahead):
        pl.semaphore_signal(barrier, inc=1, device_id={"tp": peer})

    @pl.when(is_mid)
    def _():
        pl.semaphore_signal(barrier, inc=1, device_id={"tp": behind})
        pl.semaphore_wait(barrier, 3)

    @pl.when(is_end)
    def _():
        pl.semaphore_wait(barrier, 2)

    def ag(b, kind, dev):
        return pltpu.make_async_remote_copy(
            src_ref=xbuf.at[b, c], dst_ref=xbuf.at[b, c], send_sem=asend.at[kind, b], recv_sem=arecv.at[c, b],
            device_id={"tp": dev})

    def ag_wait(b, rail):
        pltpu.make_async_copy(xbuf.at[b, rail], xbuf.at[b, rail], arecv.at[rail, b]).wait()

    def take(b):
        ag_wait(b, c)
        ag(b, 2, sib).start()

    ag(z, 0, ahead).start()

    @pl.when(is_mid)
    def _():
        ag(z, 1, behind).start()

    ag(z, 2, sib).start()

    b0 = z + s
    b1 = jnp.where(is_end, z + 2 * s, z - s)
    b2 = jnp.where(is_end, z + 3 * s, z + 2 * s)

    width = out_ref.shape[1] // PIECES

    def piece(q):
        return pl.ds(q * width, width)

    def chain(b, d, q, dev):
        return pltpu.make_async_remote_copy(
            src_ref=pbuf.at[b, c, :, piece(q)], dst_ref=rbuf.at[d, b, :, piece(q)],
            send_sem=csend.at[b, q], recv_sem=crecv.at[d, b, q], device_id={"tp": dev})

    def chain_wait(b, d, q):
        pltpu.make_async_copy(rbuf.at[d, b, :, piece(q)], rbuf.at[d, b, :, piece(q)], crecv.at[d, b, q]).wait()

    def psib(b):
        return pltpu.make_async_remote_copy(
            src_ref=pbuf.at[b, 1 - c], dst_ref=sibr.at[b], send_sem=psend.at[b], recv_sem=precv.at[b],
            device_id={"tp": sib})

    nf = act.shape[1] // 256
    rows = xbuf.shape[2]
    dim = xbuf.shape[3]

    def compute(b):
        x = xbuf[b].reshape(2 * rows, dim)
        for f in range(nf):
            cols = pl.ds(f * 256, 256)
            g = jnp.dot(x, wg[:, cols], preferred_element_type=F32)
            u = jnp.dot(x, wu[:, cols], preferred_element_type=F32)
            act[:, cols] = (silu(g) * u).astype(BF16)
        a = act[...]
        for n in range(dim // 512):
            cols = pl.ds(n * 512, 512)
            p = jnp.dot(a, wd[:, cols], preferred_element_type=F32).astype(BF16)
            pbuf[b, :, :, cols] = p.reshape(2, rows, 512)

    def step(i, carry):
        b = jnp.where(i == 0, b0, jnp.where(i == 1, b1, jnp.where(i == 2, b2, z)))

        @pl.when(i == 0)
        def _():
            take(b0)

            @pl.when(is_mid)
            def _():
                ag(b0, 1, behind).start()
                take(z - s)
                ag(z - s, 0, ahead).start()
            w_wait(wg_hbm, wg, 0)
            w_wait(wu_hbm, wu, 1)
            w_wait(wd_hbm, wd, 2)

        @pl.when(i == 1)
        def _():
            take(z + 2 * s)

            @pl.when(is_mid)
            def _():
                ag(z + 2 * s, 1, behind).start()

        @pl.when((i == 2) & is_end)
        def _():
            take(z + 3 * s)

        ag_wait(b, 1 - c)
        compute(b)
        psib(b).start()

        @pl.when(is_end & (i < 3))
        def _():
            psib(b).wait_recv()
            for q in range(PIECES):
                pbuf[b, c, :, piece(q)] = (pbuf[b, c, :, piece(q)].astype(F32) + sibr[b, :, piece(q)].astype(F32)).astype(BF16)
            for q in range(PIECES):
                chain(b, dir_a, q, ahead).start()
        return carry

    lax.fori_loop(0, 4, step, 0)

    @pl.when(is_mid)
    def _():
        f1, f2, e = z + s, z + 2 * s, z - s
        for b in (f1, f2, e):
            psib(b).wait_recv()

        def relay(b, d, q, dev):
            chain_wait(b, d, q)
            pbuf[b, c, :, piece(q)] = (pbuf[b, c, :, piece(q)].astype(F32) + sibr[b, :, piece(q)].astype(F32)
                                       + rbuf[d, b, :, piece(q)].astype(F32)).astype(BF16)
            chain(b, d, q, dev).start()

        for q in range(PIECES):
            relay(f1, dir_a, q, ahead)
        for q in range(PIECES):
            relay(f2, dir_a, q, ahead)
            relay(e, dir_b, q, behind)

    psib(z).wait_recv()
    for q in range(PIECES):
        cols = piece(q)
        chain_wait(z, dir_b, q)
        total = pbuf[z, c, :, cols].astype(F32) + sibr[z, :, cols].astype(F32) + rbuf[dir_b, z, :, cols].astype(F32)

        @pl.when(is_mid)
        def _():
            chain_wait(z, dir_a, q)

        extra = jnp.where(is_mid, rbuf[dir_a, z, :, cols].astype(F32), 0.0)
        out_ref[:, cols] = (h_ref[:, cols].astype(F32) + scale_ref[...] * (total + extra)).astype(BF16)

    ag(z, 0, ahead).wait_send()
    ag(z, 2, sib).wait_send()
    for b in (b0, b1, b2):
        ag(b, 2, sib).wait_send()
        psib(b).wait_send()
        for q in range(PIECES):
            chain(b, dir_a, q, ahead).wait_send()
    psib(z).wait_send()

    @pl.when(is_mid)
    def _():
        ag(z, 1, behind).wait_send()
        ag(z + s, 1, behind).wait_send()
        ag(z - s, 0, ahead).wait_send()
        ag(z + 2 * s, 1, behind).wait_send()


def mlp_call(h, gain, scale, w_gate, w_up, w_down, cid):
    rows, dim = h.shape
    ff = w_gate.shape[1]
    vmem = pl.BlockSpec(memory_space=pltpu.VMEM)
    hbm = pl.BlockSpec(memory_space=pl.ANY)
    dma = pltpu.SemaphoreType.DMA
    return pl.pallas_call(
        mlp_kernel,
        in_specs=[vmem, vmem, vmem, hbm, hbm, hbm],
        out_specs=vmem,
        out_shape=jax.ShapeDtypeStruct((rows, dim), BF16),
        scratch_shapes=[
            pltpu.VMEM((LINE, 2, rows, dim), BF16),
            pltpu.VMEM((dim, ff), BF16),
            pltpu.VMEM((dim, ff), BF16),
            pltpu.VMEM((ff, dim), BF16),
            pltpu.VMEM((2 * rows, ff), BF16),
            pltpu.VMEM((LINE, 2, rows, dim), BF16),
            pltpu.VMEM((LINE, rows, dim), BF16),
            pltpu.VMEM((2, LINE, rows, dim), BF16),
            dma((3,)), dma((3, LINE)), dma((2, LINE)), dma((LINE,)), dma((LINE,)),
            dma((LINE, PIECES)), dma((2, LINE, PIECES)),
        ],
        compiler_params=pltpu.CompilerParams(collective_id=cid, has_side_effects=True, vmem_limit_bytes=67043328),
        cost_estimate=pl.CostEstimate(flops=2 * 3 * rows * 8 * dim * ff, bytes_accessed=6 * dim * ff, transcendentals=0),
        name="mlp_%d" % cid,
    )(h, gain[None], scale, w_gate, w_up, w_down)


def solution(mesh):
    act_spec = P('dp', 'tp', None)
    col_spec = P(None, 'tp')
    row_spec = P('tp', None)
    layer_a = (P(), col_spec, col_spec, col_spec, row_spec, P(), col_spec, col_spec, row_spec)
    layer_b = (P(), col_spec, P(), col_spec, col_spec, P(), row_spec, P(), col_spec, col_spec, row_spec, P())
    in_specs = (act_spec, act_spec, P('dp', 'tp'), act_spec) + layer_a + layer_b
    ndp, ntp = mesh.shape['dp'], mesh.shape['tp']

    def perm(fn):
        pairs = []
        for d in range(ndp):
            for t in range(ntp):
                d2, t2 = fn(d, t)
                pairs.append((d * ntp + t, d2 * ntp + t2))
        return pairs

    def permute(x, fn):
        return lax.ppermute(x, ('dp', 'tp'), perm(fn))

    def body(hidden, vision, positions, tile_mask, ln1_a, wq_a, wk_a, wv_a, wo_a, ln2_a, wg_a, wu_a, wd_a, ln1_b, wq_b, q_norm, wk_b, wv_b, k_norm, wo_b, ln2_b, wg_b, wu_b, wd_b, xgates):
        dp = lax.axis_index('dp')
        tp = lax.axis_index('tp')
        core = tp % 2
        head_dim = q_norm.shape[0]
        model_dim = hidden.shape[2]
        toks_local = hidden.shape[1]
        kv_local = wk_a.shape[1] // head_dim
        rep_heads = wq_a.shape[1] // head_dim // kv_local
        query_shape = (model_dim, kv_local, rep_heads, head_dim)
        head_shape = (model_dim, kv_local, head_dim)
        out_shape = (kv_local, rep_heads, head_dim, model_dim)

        small = jnp.concatenate([positions[0][None], tile_mask[0].T, jnp.zeros((3, toks_local), jnp.int32)], axis=0)
        small = lax.all_gather(small, 'tp', axis=0)
        small = jnp.transpose(small, (1, 0, 2)).reshape(8, ntp * toks_local)
        pos_all = small[0]
        mask_all = small[1:5]

        gathered = gather_rows(rms_scale(hidden, ln1_a).astype(jnp.bfloat16))

        quarter = model_dim // ndp
        w_loc = jnp.concatenate([lax.dynamic_slice_in_dim(wk_b, dp * quarter, quarter, 0), lax.dynamic_slice_in_dim(wv_b, dp * quarter, quarter, 0)], axis=1)
        w_loc, gathered = lax.optimization_barrier((w_loc, gathered))
        w_own = lax.all_gather(w_loc, 'tp', axis=0)
        half = ntp // 2
        w_half = lax.dynamic_slice_in_dim(w_own, core * half, half, 0)
        b1 = permute(w_half, lambda d, t: (d ^ 1, t))
        b2 = permute(w_half, lambda d, t: (d ^ 2, t))
        d0 = permute(b1[:2], lambda d, t: (d ^ 2, t))
        d1 = permute(b2[2:], lambda d, t: (d ^ 1, t))
        sib = lambda d, t: (d, t ^ 1)
        b1s, b2s, d0s, d1s = permute(b1, sib), permute(b2, sib), permute(d0, sib), permute(d1, sib)
        tab = jnp.stack([dp, dp ^ 1, dp ^ 2, dp ^ 3, core * half, (core * half - tp + ntp) % ntp]).astype(jnp.int32)
        kv_all = kv_call(tab, vision[0], w_own, b1, b1s, b2, b2s, d0, d1, d0s, d1s, k_norm[None])
        kvs = [kv_all[0]]
        for j in range(1, ntp):
            kvs.append(permute(kv_all[j], lambda d, t, j=j: (d, (t + j) % ntp)))

        angles = pos_all.astype(jnp.float32)[None, :, None] * rope_table(head_dim)
        cos_tab = jnp.cos(angles)
        sin_tab = jnp.sin(angles)
        queries = jnp.einsum('btd,dgre->bgrte', gathered, wq_a.reshape(query_shape), preferred_element_type=jnp.float32)
        queries = rotate(queries, cos_tab[:, None, None], sin_tab[:, None, None]).astype(jnp.bfloat16)
        key_vecs = jnp.einsum('btd,dge->btge', gathered, wk_a.reshape(head_shape), preferred_element_type=jnp.float32)
        key_vecs = rotate(key_vecs, cos_tab[:, :, None], sin_tab[:, :, None]).astype(jnp.bfloat16)
        val_vecs = jnp.einsum('btd,dge->btge', gathered, wv_a.reshape(head_shape), preferred_element_type=jnp.float32).astype(jnp.bfloat16)
        context = self_attend(queries, key_vecs, val_vecs)
        partial = jnp.einsum('bgrtd,grde->bte', context, wo_a.reshape(out_shape), preferred_element_type=jnp.float32).astype(jnp.bfloat16)
        h_one = (hidden.astype(jnp.float32) + scatter_sum(partial)).astype(jnp.bfloat16)
        ones = jnp.ones((toks_local, 1), F32)
        h_two = mlp_call(h_one[0], ln2_a, ones, wg_a, wu_a, wd_a, 1)[None]

        gathered = gather_rows(rms_scale(h_two, ln1_b).astype(jnp.bfloat16))[0]
        queries = jnp.dot(gathered, wq_b, preferred_element_type=jnp.float32).reshape(-1, rep_heads * kv_local, head_dim)
        queries = rms_scale(queries, q_norm).astype(jnp.bfloat16).reshape(-1, rep_heads * kv_local * head_dim)
        tiles = jnp.stack([((tp - j + ntp) % ntp) // (ntp // 4) for j in range(ntp)])
        seen = (jnp.take(mask_all, tiles, axis=0) > 0).astype(F32).T
        context = flash_call(queries, seen, kvs)
        partial = jnp.dot(context, wo_b, preferred_element_type=jnp.float32).astype(jnp.bfloat16)[None]
        row_keep = jnp.any(tile_mask > 0, axis=-1, keepdims=True).astype(jnp.float32)
        gate_vals = jnp.tanh(xgates.astype(jnp.float32))
        h_three = (h_two.astype(jnp.float32) + gate_vals[0] * row_keep * scatter_sum(partial)).astype(jnp.bfloat16)
        return mlp_call(h_three[0], ln2_b, gate_vals[1] * row_keep[0], wg_b, wu_b, wd_b, 2)[None]

    return jax.shard_map(body, mesh=mesh, in_specs=in_specs, out_specs=act_spec, check_vma=False)
```

```python
import functools
import math
import jax
import jax.numpy as jnp
from jax import lax
from jax.experimental import pallas as pl
from jax.experimental.pallas import tpu as pltpu
from jax.sharding import PartitionSpec as P

ROPE_THETA = 500000.0
ROPE_FACTOR = 8.0
LOW_FACTOR = 1.0
HIGH_FACTOR = 4.0
ORIG_CONTEXT = 8192.0
NORM_EPS = 1e-5
MASK_VALUE = -1e30
BF16 = jnp.bfloat16
F32 = jnp.float32
MIB = 1048576
BLOCK = 256
UNROLL = 7


def rope_table(head_dim):
    low_wave = ORIG_CONTEXT / LOW_FACTOR
    high_wave = ORIG_CONTEXT / HIGH_FACTOR
    freq_list = []
    for freq_idx in range(head_dim // 2):
        base_freq = 1.0 / (ROPE_THETA ** (2.0 * freq_idx / head_dim))
        wave_len = 2.0 * math.pi / base_freq
        if wave_len > low_wave:
            freq_list.append(base_freq / ROPE_FACTOR)
        elif wave_len < high_wave:
            freq_list.append(base_freq)
        else:
            smooth = (ORIG_CONTEXT / wave_len - LOW_FACTOR) / (HIGH_FACTOR - LOW_FACTOR)
            freq_list.append((1.0 - smooth) * base_freq / ROPE_FACTOR + smooth * base_freq)
    return jnp.array(freq_list, dtype=jnp.float32)


def rms_scale(values, norm_gain):
    values = values.astype(jnp.float32)
    mean_sq = jnp.mean(values * values, axis=-1, keepdims=True)
    return values * lax.rsqrt(mean_sq + NORM_EPS) * norm_gain.astype(jnp.float32)


def rotate(values, cos_tab, sin_tab):
    half_dim = values.shape[-1] // 2
    first_half = values[..., :half_dim]
    second_half = values[..., half_dim:]
    return jnp.concatenate([first_half * cos_tab - second_half * sin_tab, second_half * cos_tab + first_half * sin_tab], axis=-1)


def self_attend(queries, key_vecs, val_vecs):
    seq_len = queries.shape[3]
    head_dim = queries.shape[4]
    scores = jnp.einsum('bgrtd,bsgd->bgrts', queries, key_vecs, preferred_element_type=jnp.float32) * (head_dim ** -0.5)
    causal = lax.broadcasted_iota(jnp.int32, (seq_len, seq_len), 0) >= lax.broadcasted_iota(jnp.int32, (seq_len, seq_len), 1)
    weights = jax.nn.softmax(jnp.where(causal, scores, MASK_VALUE), axis=-1).astype(jnp.bfloat16)
    return jnp.einsum('bgrts,bsgd->bgrtd', weights, val_vecs, preferred_element_type=jnp.float32).astype(jnp.bfloat16)


def flash_kernel(scale, q_ref, vis_ref, *refs):
    kvs, (out, s_ref, v_ref) = refs[:-3], refs[-3:]
    rows, hd = q_ref.shape
    n = kvs[0].shape[0]

    @pl.when((pl.program_id(0) == 0) & (pl.program_id(1) == 0))
    def _():
        for j, kv in enumerate(kvs):
            v_ref[j, :, :hd] = kv[:, hd:]
            v_ref[j, :, hd:] = jnp.ones((n, hd), BF16)

    q = q_ref[...]
    top = jnp.full((rows, 128), -jnp.inf, F32)
    seen = [jnp.broadcast_to(vis_ref[:, j:j + 1], (rows, 128)) > 0 for j in range(len(kvs))]
    for j, kv in enumerate(kvs):
        s = lax.dot_general(q, kv[:, :hd], (((1,), (1,)), ((), ())), preferred_element_type=F32)
        s_ref[j] = s
        best = s[:, :128]
        for k in range(1, n // 128):
            best = jnp.maximum(best, s[:, k * 128:(k + 1) * 128])
        top = jnp.where(seen[j], jnp.maximum(top, best), top)
    top = jnp.max(top, axis=-1, keepdims=True)
    acc = jnp.zeros((rows, 2 * hd), F32)
    for j in range(len(kvs)):
        shift = jnp.where(vis_ref[:, j:j + 1] > 0, top, 1e30)
        p = jnp.exp2((s_ref[j] - shift) * scale).astype(BF16)
        acc += jnp.dot(p, v_ref[j], preferred_element_type=F32)
    l = acc[:, hd:]
    out[...] = (acc[:, :hd] / jnp.where(l == 0, 1.0, l)).astype(BF16)


def flash_call(queries, seen, kvs):
    toks, width = queries.shape
    n, kw = kvs[0].shape
    hd = kw // 2
    heads = width // hd
    rows = 256
    scale = hd ** -0.5 * math.log2(math.e)
    return pl.pallas_call(
        functools.partial(flash_kernel, scale),
        grid=(toks // rows, heads),
        in_specs=[pl.BlockSpec((rows, hd), lambda i, h: (i, h)), pl.BlockSpec((rows, len(kvs)), lambda i, h: (i, 0))]
        + [pl.BlockSpec((n, kw), lambda i, h: (0, 0))] * len(kvs),
        out_specs=pl.BlockSpec((rows, hd), lambda i, h: (i, h)),
        out_shape=jax.ShapeDtypeStruct((toks, width), BF16),
        scratch_shapes=[pltpu.VMEM((len(kvs), rows, n), F32), pltpu.VMEM((len(kvs), n, kw), BF16)],
        compiler_params=pltpu.CompilerParams(vmem_limit_bytes=48 * MIB),
        cost_estimate=pl.CostEstimate(flops=4 * toks * width * n * len(kvs), bytes_accessed=8 * MIB, transcendentals=toks * heads * n * len(kvs)),
        name="cross_flash",
    )(queries, seen, *kvs)


LINE = 4
PIECES = 4
VMEM_SPEC = pl.BlockSpec(memory_space=pltpu.VMEM)
ANY_SPEC = pl.BlockSpec(memory_space=pl.ANY)
DMA = pltpu.SemaphoreType.DMA


class Roles:
    def __init__(self):
        t = lax.axis_index("tp")
        self.t = t
        self.c = lax.rem(t, 2)
        self.o = 1 - self.c
        z = lax.div(t, 2)
        self.z = z
        up_side = z < LINE // 2
        s = jnp.where(up_side, 1, -1)
        self.is_end = (z == 0) | (z == LINE - 1)
        self.is_mid = jnp.logical_not(self.is_end)
        self.sib = t + self.o - self.c
        self.ahead = t + s + s
        self.behind = t - s - s
        self.dir_a = jnp.where(up_side, 0, 1)
        self.dir_b = 1 - self.dir_a
        self.near, self.far, self.back = z + s, z + s + s, z - s
        self.last = self.far + s
        self.arrive = (self.near, jnp.where(self.is_end, self.far, self.back), jnp.where(self.is_end, self.last, self.far))

    def mid(self, fn):
        pl.when(self.is_mid)(fn)

    def end(self, fn):
        pl.when(self.is_end)(fn)

    def meet(self, others=()):
        barrier = pltpu.get_barrier_semaphore()
        for peer in (self.sib, self.ahead):
            pl.semaphore_signal(barrier, device_id={"tp": peer})
        for peer in others:
            pl.semaphore_signal(barrier, device_id={"dp": peer})
        n = len(others)

        def mid_meet():
            pl.semaphore_signal(barrier, device_id={"tp": self.behind})
            pl.semaphore_wait(barrier, n + 3)

        self.mid(mid_meet)
        self.end(lambda: pl.semaphore_wait(barrier, n + 2))


def pick(i, values):
    out = values[-1]
    for n, v in enumerate(values[:-1]):
        out = jnp.where(i == n, v, out)
    return out


def norm_rows(h_ref, gain_ref):
    return rms_scale(h_ref[:], gain_ref[:]).astype(BF16)


def landed(ref, sem):
    pltpu.make_async_copy(ref, ref, sem).wait()


class Gather:
    def __init__(self, roles, *sets):
        self.r, self.sets = roles, sets

    def copies(self, b, way, dev):
        c = self.r.c
        return [pltpu.make_async_remote_copy(
            src_ref=buf.at[b, c], dst_ref=buf.at[b, c], send_sem=send.at[way, b], recv_sem=recv.at[c, b],
            device_id={"tp": dev}) for buf, send, recv in self.sets]

    def go(self, b, way, dev):
        for cp in self.copies(b, way, dev):
            cp.start()

    def ahead(self, b):
        self.go(b, 0, self.r.ahead)

    def behind(self, b):
        self.go(b, 1, self.r.behind)

    def across(self, b):
        self.go(b, 2, self.r.sib)

    def wait(self, b, rail):
        for buf, _, recv in self.sets:
            landed(buf.at[b, rail], recv.at[rail, b])

    def ready(self, b):
        self.wait(b, self.r.o)

    def take(self, b):
        self.wait(b, self.r.c)
        self.across(b)

    def begin(self):
        z = self.r.z
        self.ahead(z)
        self.r.mid(lambda: self.behind(z))
        self.across(z)

    def first(self):
        r = self.r
        self.take(r.near)

        def more():
            self.behind(r.near)
            self.take(r.back)
            self.ahead(r.back)

        r.mid(more)

    def second(self):
        self.take(self.r.far)
        self.r.mid(lambda: self.behind(self.r.far))

    def third(self):
        self.r.end(lambda: self.take(self.r.last))

    def finish(self):
        r = self.r

        def sent(b, way, dev):
            for cp in self.copies(b, way, dev):
                cp.wait_send()

        sent(r.z, 0, r.ahead)
        for b in (r.z, *r.arrive):
            sent(b, 2, r.sib)

        def more():
            for b in (r.z, r.near, r.far):
                sent(b, 1, r.behind)
            sent(r.back, 0, r.ahead)

        r.mid(more)


class Sum:
    def __init__(self, roles, pbuf, sibr, rbuf, psend, precv, csend, crecv):
        self.r, self.pbuf, self.sibr, self.rbuf = roles, pbuf, sibr, rbuf
        self.psend, self.precv, self.csend, self.crecv = psend, precv, csend, crecv
        self.width = pbuf.shape[-1] // PIECES

    def cols(self, q):
        return pl.ds(pl.multiple_of(q * self.width, self.width), self.width)

    def pair(self, b, q):
        return pltpu.make_async_remote_copy(
            src_ref=self.pbuf.at[b, self.r.o, :, self.cols(q)], dst_ref=self.sibr.at[b, :, self.cols(q)],
            send_sem=self.psend.at[b, q], recv_sem=self.precv.at[b, q], device_id={"tp": self.r.sib})

    def chain(self, b, d, q, dev):
        return pltpu.make_async_remote_copy(
            src_ref=self.pbuf.at[b, self.r.c, :, self.cols(q)], dst_ref=self.rbuf.at[d, b, :, self.cols(q)],
            send_sem=self.csend.at[b, q], recv_sem=self.crecv.at[d, b, q], device_id={"tp": dev})

    def both(self, b, q):
        cols = self.cols(q)
        landed(self.sibr.at[b, :, cols], self.precv.at[b, q])
        return self.pbuf[b, self.r.c, :, cols].astype(F32) + self.sibr[b, :, cols].astype(F32)

    def arrived(self, d, b, q):
        ref = self.rbuf.at[d, b, :, self.cols(q)]
        landed(ref, self.crecv.at[d, b, q])
        return ref[:].astype(F32)

    def pass_on(self, b, d, q, dev, first):
        total = self.both(b, q)
        if not first:
            total = total + self.arrived(d, b, q)
        self.pbuf[b, self.r.c, :, self.cols(q)] = total.astype(BF16)
        self.chain(b, d, q, dev).start()

    def from_end(self, b):
        for q in range(PIECES):
            self.pass_on(b, self.r.dir_a, q, self.r.ahead, True)

    def relay(self, groups):
        r = self.r

        def run():
            for group in groups:
                for q in range(PIECES):
                    for b in group:
                        if b is r.back:
                            self.pass_on(b, r.dir_b, q, r.behind, False)
                        else:
                            self.pass_on(b, r.dir_a, q, r.ahead, False)

        r.mid(run)

    def finish(self, h_ref, scale_ref, out_ref):
        r = self.r
        for q in range(PIECES):
            cols = self.cols(q)
            out_ref[:, cols] = self.both(r.z, q) + self.arrived(r.dir_b, r.z, q)

            def more():
                out_ref[:, cols] += self.arrived(r.dir_a, r.z, q)

            r.mid(more)
        h_ref[:] = (h_ref[:].astype(F32) + scale_ref[:] * out_ref[:]).astype(BF16)
        for b in (r.z, *r.arrive):
            for q in range(PIECES):
                self.pair(b, q).wait_send()
        for b in r.arrive:
            for q in range(PIECES):
                self.chain(b, r.dir_a, q, r.ahead).wait_send()


def sum_scratch(rows, dim):
    two = DMA((LINE, PIECES))
    return [
        pltpu.VMEM((LINE, 2, rows, dim), BF16), pltpu.VMEM((LINE, rows, dim), BF16), pltpu.VMEM((2, LINE, rows, dim), BF16),
        two, two, two, DMA((2, LINE, PIECES)),
    ]


def gather_scratch():
    return [DMA((3, LINE)), DMA((2, LINE))]


def comm_params(cid, mib):
    return pltpu.CompilerParams(collective_id=cid, has_side_effects=True, vmem_limit_bytes=int(mib * MIB))


def silu(x):
    return x / (1.0 + jnp.exp(-x))


def mlp_kernel(h_ref, gain_ref, scale_ref, wg_hbm, wu_hbm, wd_hbm, out_ref, xbuf, wg, wu, wd, act, total, asend, arecv, wsem, *sums):
    r = Roles()
    gather = Gather(r, (xbuf, asend, arecv))
    sums = Sum(r, *sums)
    weights = ((wg_hbm, wg, wsem.at[0]), (wu_hbm, wu, wsem.at[1]), (wd_hbm, wd, wsem.at[2]))
    for src, dst, sem in weights:
        n = src.shape[0] // LINE
        for i in range(LINE):
            pltpu.make_async_copy(src.at[pl.ds(i * n, n)], dst.at[pl.ds(i * n, n)], sem).start()
    xbuf[r.z, r.c] = norm_rows(h_ref, gain_ref)
    r.meet()
    gather.begin()
    rows, dim = h_ref.shape

    def compute(b):
        x = xbuf[b].reshape(2 * rows, dim)

        def inner(f, carry):
            cols = pl.ds(pl.multiple_of(f * BLOCK, BLOCK), BLOCK)
            g = jnp.dot(x, wg[:, cols], preferred_element_type=F32)
            u = jnp.dot(x, wu[:, cols], preferred_element_type=F32)
            act[:, cols] = (silu(g) * u).astype(BF16)
            return carry

        lax.fori_loop(0, act.shape[1] // BLOCK, inner, 0, unroll=UNROLL)

        def outer(q, carry):
            p = jnp.dot(act[:], wd[:, sums.cols(q)], preferred_element_type=F32).astype(BF16)
            sums.pbuf[b, :, :, sums.cols(q)] = p.reshape(2, rows, sums.width)
            sums.pair(b, q).start()
            return carry

        lax.fori_loop(0, PIECES, outer, 0)

    def step(i, carry):
        @pl.when(i == 0)
        def _():
            gather.first()
            for src, dst, sem in weights:
                pltpu.make_async_copy(src, dst, sem).wait()

        pl.when(i == 1)(gather.second)
        pl.when(i == 2)(gather.third)
        pl.when(i == 3)(lambda: sums.relay(((r.near,),)))
        b = pick(i, (*r.arrive, r.z))
        gather.ready(b)
        compute(b)
        pl.when(r.is_end & (i < 3))(lambda: sums.from_end(b))
        return carry

    lax.fori_loop(0, LINE, step, 0)
    sums.relay(((r.far, r.back),))
    out_ref[:] = h_ref[:]
    sums.finish(out_ref, scale_ref, total)
    gather.finish()


def mlp_call(h, gain, scale, w_gate, w_up, w_down, cid):
    rows, dim = h.shape
    ff = w_gate.shape[1]
    return pl.pallas_call(
        mlp_kernel,
        in_specs=[VMEM_SPEC] * 3 + [ANY_SPEC] * 3,
        out_specs=VMEM_SPEC,
        out_shape=jax.ShapeDtypeStruct((rows, dim), BF16),
        scratch_shapes=[
            pltpu.VMEM((LINE, 2, rows, dim), BF16),
            pltpu.VMEM((dim, ff), BF16), pltpu.VMEM((dim, ff), BF16), pltpu.VMEM((ff, dim), BF16),
            pltpu.VMEM((2 * rows, ff), BF16), pltpu.VMEM((rows, dim), F32),
        ] + gather_scratch() + [DMA((3,))] + sum_scratch(rows, dim),
        compiler_params=comm_params(cid, 63.9),
        cost_estimate=pl.CostEstimate(flops=48 * rows * dim * ff, bytes_accessed=6 * dim * ff, transcendentals=0),
    )(h, gain[None], scale, w_gate, w_up, w_down)


def start_kernel(h_ref, gain_ref, small_ref, w_ref, kgain_ref, wq_hbm, wk_hbm, wv_hbm, vis_hbm, q_out, k_out, v_out, small_out, *rest):
    kv_outs, rest = rest[:2 * LINE], rest[2 * LINE:]
    w_all, acc, vis, wq, wk, wv, xbuf, xsend, xrecv, isend, irecv, lsem, zsend, zrecv, ysend, yrecv, hsend, hrecv, dsend, drecv, ssend, srecv = rest
    r = Roles()
    z, c, t, s_near, s_far = r.z, r.c, r.t, r.near, r.far
    b0, b1, b2 = r.arrive
    d = lax.axis_index("dp")
    dd = w_all.shape[0] - 1 - d
    dy = d + 1 - 2 * lax.rem(d, 2)
    dx = w_all.shape[0] - 1 - dy
    gather = Gather(r, (xbuf, xsend, xrecv), (small_out, isend, irecv))

    xbuf[z, c] = norm_rows(h_ref, gain_ref)
    small_out[z, c] = small_ref[:]
    local = [pltpu.make_async_copy(src, dst, lsem.at[i]) for i, (src, dst) in enumerate(
        ((vis_hbm, vis), (wq_hbm, wq), (wk_hbm, wk), (wv_hbm, wv)))]
    for cp in local:
        cp.start()
    r.meet((dy, dx))

    def piece(q, b):
        return w_all.at[q, 2 * b + c]

    def send(q, b, ssem, rsem, peer, src=None):
        return pltpu.make_async_remote_copy(
            src_ref=piece(q, b) if src is None else src, dst_ref=piece(q, b), send_sem=ssem, recv_sem=rsem, device_id=peer)

    def ahead(b, src=None):
        return send(d, b, zsend.at[0, b], zrecv.at[b], {"tp": r.ahead}, src)

    def behind(b, src=None):
        return send(d, b, zsend.at[1, b], zrecv.at[b], {"tp": r.behind}, src)

    def plane(b, src=None):
        return [send(d, b, ysend.at[b], yrecv.at[b], {"dp": dy}, src), send(d, b, hsend.at[b], hrecv.at[b], {"dp": dx}, src)]

    def diag(b, q, peer):
        return send(q, b, dsend.at[b], drecv.at[b], {"dp": peer})

    def across(b, q, k, src=None):
        return send(q, b, ssend.at[k, b], srecv.at[k, b], {"tp": r.sib}, src)

    def spread(b, src=None):
        for cp in plane(b, src):
            cp.start()
        across(b, d, 0, src).start()

    def z_arrived(b):
        landed(piece(d, b), zrecv.at[b])

    def plane_arrived(b):
        even = lax.rem(b, 2) == 0
        landed(piece(dy, b), yrecv.at[b])
        pl.when(even)(lambda: diag(b, dy, dx).start())
        across(b, dy, 1).start()
        landed(piece(dx, b), hrecv.at[b])
        pl.when(jnp.logical_not(even))(lambda: diag(b, dx, dy).start())
        across(b, dx, 2).start()

    def diag_arrived(b):
        landed(piece(dd, b), drecv.at[b])
        across(b, dd, 3).start()

    rows, dim = h_ref.shape
    quarter = w_ref.shape[0]

    def kv_add(*pieces):
        for k, q, b in pieces:
            landed(w_all.at[q, 2 * b + r.o], srecv.at[k, b])

        def one(i, carry):
            n = lax.div(i, 2)
            q = pick(n, [p[1] for p in pieces])
            head = 2 * pick(n, [p[2] for p in pieces]) + lax.rem(i, 2)
            acc[head] += jnp.dot(vis[:, pl.ds(pl.multiple_of(q * quarter, quarter), quarter)], w_all[q, head], preferred_element_type=F32)
            return carry

        lax.fori_loop(0, 2 * len(pieces), one, 0)

    def products(*blocks):
        def one(i, carry):
            b = pick(i, blocks)
            x = xbuf[b].reshape(2 * rows, dim)
            at = pl.ds(pl.multiple_of(b * 2 * rows, 2 * rows), 2 * rows)
            for w, out in ((wq, q_out), (wk, k_out), (wv, v_out)):
                out[at, :] = jnp.dot(x, w[:], preferred_element_type=F32)
            return carry

        lax.fori_loop(0, len(blocks), one, 0)

    ahead(z, w_ref).start()
    r.mid(lambda: behind(z, w_ref).start())
    spread(z, w_ref)
    w_all[d, t] = w_ref[:]

    def clear(i, carry):
        acc[i] = jnp.zeros(acc.shape[1:], F32)
        return carry

    lax.fori_loop(0, 2 * LINE, clear, 0)
    for cp in local:
        cp.wait()

    z_arrived(b0)

    def more():
        behind(b0).start()
        z_arrived(r.back)
        ahead(r.back).start()

    r.mid(more)
    gather.begin()
    spread(b0)
    r.mid(lambda: spread(r.back))
    plane_arrived(z)
    z_arrived(s_far)
    r.mid(lambda: behind(s_far).start())
    spread(s_far)
    plane_arrived(b0)
    gather.first()

    def end_more():
        z_arrived(r.last)
        spread(r.last)

    r.end(end_more)
    plane_arrived(b1)
    kv_add((0, d, z), (0, d, b0), (1, dy, z), (2, dx, z))
    gather.second()
    kv_add((0, d, b1), (1, dy, b0), (2, dx, b0))
    plane_arrived(b2)
    kv_add((0, d, b2), (1, dy, b1), (2, dx, b1))
    diag_arrived(z)
    diag_arrived(b0)
    kv_add((1, dy, b2), (2, dx, b2), (3, dd, z), (3, dd, b0))
    gather.third()
    for b in (z, b0, b1, b2):
        gather.ready(b)
    products(z, b0, b1, b2)
    diag_arrived(b1)
    diag_arrived(b2)
    kv_add((3, dd, b1), (3, dd, b2))
    hd = kgain_ref.shape[1]
    for j, out in enumerate(kv_outs):
        head = lax.rem(t + j, 2 * LINE)

        def store(i, carry):
            at = pl.ds(pl.multiple_of(i * 2 * rows, 2 * rows), 2 * rows)
            out[at, :hd] = rms_scale(acc[head, at, :hd], kgain_ref[:]).astype(BF16)
            out[at, hd:] = acc[head, at, hd:].astype(BF16)
            return carry

        lax.fori_loop(0, out.shape[0] // (2 * rows), store, 0)

    for b in (z, b0, b1, b2):
        for k, q in enumerate((d, dy, dx, dd)):
            across(b, q, k).wait_send()
        for cp in plane(b):
            cp.wait_send()
        diag(b, dy, dx).wait_send()
    gather.finish()
    ahead(z).wait_send()

    def mid_sent():
        for b in (z, s_near, s_far):
            behind(b).wait_send()
        ahead(r.back).wait_send()

    r.mid(mid_sent)


def start_call(h, gain, small, w_loc, kgain, wq, wk, wv, vision, ndp, cid):
    rows, dim = h.shape
    heads = 2 * LINE
    toks = rows * heads
    quarter, width = w_loc.shape
    vtoks = vision.shape[0]
    line, four = DMA((LINE,)), DMA((4, LINE))
    return pl.pallas_call(
        start_kernel,
        in_specs=[VMEM_SPEC] * 5 + [ANY_SPEC] * 4,
        out_specs=[VMEM_SPEC] * (4 + heads),
        out_shape=[jax.ShapeDtypeStruct((toks, w.shape[1]), F32) for w in (wq, wk, wv)]
        + [jax.ShapeDtypeStruct((LINE, 2) + small.shape, jnp.int32)]
        + [jax.ShapeDtypeStruct((vtoks, width), BF16)] * heads,
        scratch_shapes=[
            pltpu.VMEM((ndp, heads, quarter, width), BF16),
            pltpu.VMEM((heads, vtoks, width), F32),
        ] + [pltpu.VMEM(w.shape, BF16) for w in (vision, wq, wk, wv)]
        + [pltpu.VMEM((LINE, 2, rows, dim), BF16)] + gather_scratch() + gather_scratch()
        + [DMA((4,)), DMA((2, LINE)), line, line, line, line, line, line, line, four, four],
        compiler_params=comm_params(cid, 60),
        cost_estimate=pl.CostEstimate(flops=toks * dim * wq.shape[1], bytes_accessed=30 * MIB, transcendentals=0),
        name="start",
    )(h, gain[None], small, w_loc, kgain[None], wq, wk, wv, vision)


def query_kernel(h_ref, gain_ref, hgain_ref, wq_hbm, out_ref, xbuf, wq, wsem, asend, arecv):
    load = pltpu.make_async_copy(wq_hbm, wq, wsem.at[0])
    load.start()
    r = Roles()
    gather = Gather(r, (xbuf, asend, arecv))
    rows, dim = h_ref.shape
    hd = hgain_ref.shape[1]
    xbuf[r.z, r.c] = norm_rows(h_ref, gain_ref)
    r.meet()
    gather.begin()
    load.wait()

    def step(i, carry):
        pl.when(i == 1)(gather.first)
        pl.when(i == 2)(gather.second)
        pl.when(i == 3)(gather.third)
        b = pick(i, (r.z, *r.arrive))
        gather.ready(b)
        y = jnp.dot(xbuf[b].reshape(2 * rows, dim), wq[:], preferred_element_type=F32)
        at = pl.ds(pl.multiple_of(b * 2 * rows, 2 * rows), 2 * rows)
        for n in range(y.shape[1] // hd):
            cols = slice(n * hd, n * hd + hd)
            out_ref[at, cols] = rms_scale(y[:, cols], hgain_ref[:]).astype(BF16)
        return carry

    lax.fori_loop(0, LINE, step, 0)
    gather.finish()


def query_call(h, gain, hgain, wq, cid):
    rows, dim = h.shape
    toks = rows * 2 * LINE
    return pl.pallas_call(
        query_kernel,
        in_specs=[VMEM_SPEC] * 3 + [ANY_SPEC],
        out_specs=VMEM_SPEC,
        out_shape=jax.ShapeDtypeStruct((toks, wq.shape[1]), BF16),
        scratch_shapes=[pltpu.VMEM((LINE, 2, rows, dim), BF16), pltpu.VMEM(wq.shape, BF16), DMA((1,))] + gather_scratch(),
        compiler_params=comm_params(cid, 24),
        cost_estimate=pl.CostEstimate(flops=2 * toks * dim * wq.shape[1], bytes_accessed=10 * MIB, transcendentals=0),
        name="query",
    )(h, gain[None], hgain[None], wq)


def output_kernel(h_ref, scale_ref, ctx, wo_hbm, out_ref, wo, wsem, total, *sums):
    load = pltpu.make_async_copy(wo_hbm, wo, wsem.at[0])
    load.start()
    r = Roles()
    sums = Sum(r, *sums)
    rows = h_ref.shape[0]
    r.meet()
    load.wait()
    order = (jnp.where(r.is_end, r.last, r.far), jnp.where(r.is_end, r.far, r.near), jnp.where(r.is_end, r.near, r.back), r.z)

    def step(i, carry):
        b = pick(i, order)
        x = ctx[pl.ds(pl.multiple_of(b * 2 * rows, 2 * rows), 2 * rows), :]

        def outer(q, carry):
            p = jnp.dot(x, wo[:, sums.cols(q)], preferred_element_type=F32).astype(BF16)
            sums.pbuf[b, :, :, sums.cols(q)] = p.reshape(2, rows, sums.width)
            sums.pair(b, q).start()
            return carry

        lax.fori_loop(0, PIECES, outer, 0)
        pl.when(r.is_end & (i < 3))(lambda: sums.from_end(b))
        return carry

    lax.fori_loop(0, LINE, step, 0)
    sums.relay(((r.far, r.back), (r.near,)))
    out_ref[:] = h_ref[:]
    sums.finish(out_ref, scale_ref, total)


def output_call(h, scale, ctx, wo, cid):
    rows, dim = h.shape
    return pl.pallas_call(
        output_kernel,
        in_specs=[VMEM_SPEC] * 3 + [ANY_SPEC],
        out_specs=VMEM_SPEC,
        out_shape=jax.ShapeDtypeStruct((rows, dim), BF16),
        scratch_shapes=[pltpu.VMEM(wo.shape, BF16), DMA((1,)), pltpu.VMEM((rows, dim), F32)] + sum_scratch(rows, dim),
        compiler_params=comm_params(cid, 32),
        cost_estimate=pl.CostEstimate(flops=2 * rows * dim * wo.shape[0], bytes_accessed=10 * MIB, transcendentals=0),
        name="output",
    )(h, scale, ctx, wo)


def solution(mesh):
    act_spec = P('dp', 'tp', None)
    col_spec = P(None, 'tp')
    row_spec = P('tp', None)
    layer_a = (P(), col_spec, col_spec, col_spec, row_spec, P(), col_spec, col_spec, row_spec)
    layer_b = (P(), col_spec, P(), col_spec, col_spec, P(), row_spec, P(), col_spec, col_spec, row_spec, P())
    in_specs = (act_spec, act_spec, P('dp', 'tp'), act_spec) + layer_a + layer_b
    ndp, ntp = mesh.shape['dp'], mesh.shape['tp']

    def perm(fn):
        pairs = []
        for d in range(ndp):
            for t in range(ntp):
                d2, t2 = fn(d, t)
                pairs.append((d * ntp + t, d2 * ntp + t2))
        return pairs

    def permute(x, fn):
        return lax.ppermute(x, ('dp', 'tp'), perm(fn))

    def body(hidden, vision, positions, tile_mask, ln1_a, wq_a, wk_a, wv_a, wo_a, ln2_a, wg_a, wu_a, wd_a, ln1_b, wq_b, q_norm, wk_b, wv_b, k_norm, wo_b, ln2_b, wg_b, wu_b, wd_b, xgates):
        dp = lax.axis_index('dp')
        tp = lax.axis_index('tp')
        head_dim = q_norm.shape[0]
        model_dim = hidden.shape[2]
        toks_local = hidden.shape[1]
        kv_local = wk_a.shape[1] // head_dim
        rep_heads = wq_a.shape[1] // head_dim // kv_local

        quarter = model_dim // ndp
        w_loc = jnp.concatenate([lax.dynamic_slice_in_dim(wk_b, dp * quarter, quarter, 0), lax.dynamic_slice_in_dim(wv_b, dp * quarter, quarter, 0)], axis=1)
        small = jnp.concatenate([positions[0][None], tile_mask[0].T, jnp.zeros((3, toks_local), jnp.int32)], axis=0)
        small = jnp.pad(small, ((0, 0), (0, 128 - toks_local)))
        queries, key_vecs, val_vecs, small, *kvs = start_call(hidden[0], ln1_a, small, w_loc, k_norm, wq_a, wk_a, wv_a, vision[0], ndp, 3)
        small = jnp.transpose(small.reshape(ntp, 8, 128)[:, :, :toks_local], (1, 0, 2)).reshape(8, ntp * toks_local)
        pos_all = small[0]
        mask_all = small[1:5]
        for j in range(1, ntp):
            kvs[j] = permute(kvs[j], lambda d, t, j=j: (d, (t + j) % ntp))

        angles = pos_all.astype(jnp.float32)[None, :, None] * rope_table(head_dim)
        cos_tab = jnp.cos(angles)
        sin_tab = jnp.sin(angles)
        queries = queries.reshape(1, -1, kv_local, rep_heads, head_dim).transpose(0, 2, 3, 1, 4)
        queries = rotate(queries, cos_tab[:, None, None], sin_tab[:, None, None]).astype(jnp.bfloat16)
        key_vecs = key_vecs.reshape(1, -1, kv_local, head_dim)
        key_vecs = rotate(key_vecs, cos_tab[:, :, None], sin_tab[:, :, None]).astype(jnp.bfloat16)
        val_vecs = val_vecs.reshape(1, -1, kv_local, head_dim).astype(jnp.bfloat16)
        context = self_attend(queries, key_vecs, val_vecs)
        context = context[0].transpose(2, 0, 1, 3).reshape(-1, wo_a.shape[0])
        ones = jnp.ones((toks_local, 1), F32)
        h_one = output_call(hidden[0], ones, context, wo_a, 6)
        h_two = mlp_call(h_one, ln2_a, ones, wg_a, wu_a, wd_a, 1)

        queries = query_call(h_two, ln1_b, q_norm, wq_b, 4)
        tiles = jnp.stack([((tp - j + ntp) % ntp) // (ntp // 4) for j in range(ntp)])
        seen = (jnp.take(mask_all, tiles, axis=0) > 0).astype(F32).T
        context = flash_call(queries, seen, kvs)
        row_keep = jnp.any(tile_mask > 0, axis=-1, keepdims=True).astype(jnp.float32)
        gate_vals = jnp.tanh(xgates.astype(jnp.float32))
        h_three = output_call(h_two, gate_vals[0] * row_keep[0], context, wo_b, 5)
        return mlp_call(h_three, ln2_b, gate_vals[1] * row_keep[0], wg_b, wu_b, wd_b, 2)[None]

    return jax.shard_map(body, mesh=mesh, in_specs=in_specs, out_specs=act_spec, check_vma=False)
```
